32 devices in a mesh: prow: 8 (over z, y), pcol: 4 (over x, core).
Axes of the slice: x: 2, y: 2, z: 4, core: 2. Of those that a mesh axis runs over, the one named last changes fastest.
Arguments:
- iface_tiles: int32 [32, 16], replicated, may hold values from 0 to 63, as said below
- interior_sizes: int32 [32], P(('prow', 'pcol')), may hold values from 128 to 512
- coupling: float32 [32, 512, 2048], P(('prow', 'pcol')), may hold values from -0.25 to 0.25
- factor_inverse: float32 [32, 512, 512], P(('prow', 'pcol')), as said below
- interface_block: float32 [8, 8, 4, 16, 128, 128], P('prow', None, 'pcol'), as said below
Outputs:
- schur: float32 [8, 8, 4, 16, 128, 128], P('prow', None, 'pcol')
- panel: float32 [8, 8, 128, 128], P('prow', None, 'pcol')
The draws below stay inside these ranges and needn't reach their ends.
Inputs may be any that keep to these rules, and one draw needn't show every extreme that they name: `iface_tiles`: each row holds 16 distinct tile numbers; for every r, exactly 2 of them are r modulo 8; every tile number stands in exactly 8 rows. `factor_inverse`: each matrix is lower triangular with a diagonal between 0.25 and 1. `interface_block`: diagonal entries lie between 80 and 160; other entries are of order one.
All inputs are finite; a program needn't handle non-finite values.
Results may differ from the reference program's by a relative error of at most 0.0001.
Values sent between devices are 32-bit elements; how exact they have to be, the bound alone decides.
A program may use at most 128 MiB of HBM per device.

```python
import jax
import jax.numpy as jnp
from jax import lax

IFACE = 2048
TILE = 128
NI = 512
LR_DEV = 8
GT = 16
NT = 64
LC = 16
SUBDOMAINS = 32
N_PROW = 8
N_PCOL = 4


def shuffle_row(row_key, values):
    return jax.random.permutation(row_key, values)


def draw_iface_tiles(key, part):
    rows_per = IFACE // TILE // N_PROW
    key_list = jax.random.split(jax.random.fold_in(key, 11), N_PROW)
    orders = jax.vmap(shuffle_row)(key_list, jnp.broadcast_to(jnp.arange(SUBDOMAINS, dtype=jnp.int32), (N_PROW, SUBDOMAINS)))
    quotient = (rows_per * orders.T[:, :, None] + jnp.arange(rows_per, dtype=jnp.int32)[None, None, :]) % LR_DEV
    tile_ids = quotient * N_PROW + jnp.arange(N_PROW, dtype=jnp.int32)[None, :, None]
    tile_ids = tile_ids.reshape(SUBDOMAINS, rows_per * N_PROW).astype(jnp.int32)
    shuffle_keys = jax.random.split(jax.random.fold_in(key, 12), SUBDOMAINS)
    return jax.vmap(shuffle_row)(shuffle_keys, tile_ids).astype(jnp.int32)


def draw_factor_inverse(key, part):
    first_key = jax.random.fold_in(key, 21)
    second_key = jax.random.fold_in(key, 22)
    shape = (SUBDOMAINS, NI, NI)
    noise = jax.random.normal(first_key, shape, jnp.float32) * (0.5 / NI ** 0.5)
    diagonal = jax.random.uniform(second_key, (SUBDOMAINS, NI), jnp.float32, 0.5, 1.0)
    lower = jnp.tril(noise, -1)
    eye_mask = jnp.eye(NI, dtype=jnp.float32)[None, :, :]
    return (lower + eye_mask * diagonal[:, :, None]).astype(jnp.float32)


def draw_interface_block(key, part):
    local_cols = LR_DEV * N_PROW // N_PCOL
    shape = (N_PROW, LR_DEV, N_PCOL, local_cols, TILE, TILE)
    first_key = jax.random.fold_in(key, 31)
    second_key = jax.random.fold_in(key, 32)
    noise = jax.random.normal(first_key, shape, jnp.float32) * 0.5
    diagonal = jax.random.uniform(second_key, shape, jnp.float32, 80.0, 160.0)
    prow_ids = jnp.arange(N_PROW, dtype=jnp.int32)[:, None, None, None, None, None]
    row_tiles = jnp.arange(LR_DEV, dtype=jnp.int32)[None, :, None, None, None, None]
    pcol_ids = jnp.arange(N_PCOL, dtype=jnp.int32)[None, None, :, None, None, None]
    col_tiles = jnp.arange(local_cols, dtype=jnp.int32)[None, None, None, :, None, None]
    inner_rows = jnp.arange(TILE, dtype=jnp.int32)[None, None, None, None, :, None]
    inner_cols = jnp.arange(TILE, dtype=jnp.int32)[None, None, None, None, None, :]
    global_row = (row_tiles * N_PROW + prow_ids) * TILE + inner_rows
    global_col = (col_tiles * N_PCOL + pcol_ids) * TILE + inner_cols
    return jnp.where(global_row == global_col, diagonal, noise).astype(jnp.float32)


def set_ends(entries, stream_key, low, top_value):
    shape = entries.shape
    place = [jax.random.randint(jax.random.fold_in(stream_key, axis), (), 0, shape[axis]) for axis in range(len(shape))]
    entries = entries.at[tuple(place)].set(low)
    longest = shape.index(max(shape))
    place[longest] = (place[longest] + 1) % shape[longest]
    return entries.at[tuple(place)].set(top_value)


def block_scale(stream_key, extent, pieces, smallest, top_value):
    def one(position, shards_of):
        heights = jax.random.uniform(jax.random.fold_in(jax.random.fold_in(stream_key, 6), position), (shards_of,), jnp.float32, smallest / len(pieces), top_value / len(pieces))
        return jnp.repeat(jnp.exp(heights), extent[position] // shards_of).reshape((-1,) + (1,) * (len(extent) - position - 1))

    loudness = one(*pieces[0])
    for cut in pieces[1:]:
        loudness = loudness * one(*cut)
    return loudness


def centred(key, extent, deviation, limit, shards=(), kind=jnp.bfloat16):
    gain = block_scale(key, extent, shards, -0.22, 0.18) if shards else 1.0
    array = jax.random.normal(key, extent, jnp.float32) * deviation * gain
    return jnp.minimum(jnp.maximum(array, -limit), limit).astype(kind)


def setup_inputs(seed: int = 0) -> dict:
    key_of = jax.random.split(jax.random.key(seed), 6)
    iface_tiles = draw_iface_tiles(jax.random.fold_in(key_of[5], 71), 0)
    interior_sizes = set_ends(jax.random.randint(key_of[1], (SUBDOMAINS,), NI // 4, NI + 1), jax.random.fold_in(key_of[1], 1), NI // 4, NI).astype(jnp.int32)
    coupling = centred(key_of[2], (SUBDOMAINS, NI, IFACE), NI ** -0.5, 0.25, ((0, 32),), jnp.float32)
    factor_inverse = draw_factor_inverse(jax.random.fold_in(key_of[5], 71), 0)
    interface_block = draw_interface_block(jax.random.fold_in(key_of[5], 71), 0)
    return {"iface_tiles": iface_tiles, "interior_sizes": interior_sizes, "coupling": coupling, "factor_inverse": factor_inverse, "interface_block": interface_block}


def reference(iface_tiles, interior_sizes, coupling, factor_inverse, interface_block):
    grid_tiles = interface_block.transpose(1, 0, 3, 2, 4, 5).reshape(NT, NT, TILE, TILE)

    def add_domain(index, running):
        live_count = interior_sizes[index]
        row_live = (jnp.arange(NI, dtype=jnp.int32) < live_count)[:, None]
        masked = jnp.where(row_live, coupling[index], 0.0)
        weighted = jnp.dot(factor_inverse[index].astype(jnp.float32), masked.astype(jnp.float32), precision=lax.Precision.HIGHEST, preferred_element_type=jnp.float32)
        weighted = jnp.where(row_live, weighted, 0.0)
        gram = jnp.dot(weighted.T.astype(jnp.float32), weighted.astype(jnp.float32), precision=lax.Precision.HIGHEST, preferred_element_type=jnp.float32)
        tiled = gram.reshape(GT, TILE, GT, TILE).transpose(0, 2, 1, 3)
        tile_ids = iface_tiles[index].astype(jnp.int32)
        return running.at[tile_ids[:, None], tile_ids[None, :]].add(-tiled)
    grid_tiles = lax.fori_loop(0, SUBDOMAINS, add_domain, grid_tiles)
    schur = grid_tiles.reshape(LR_DEV, N_PROW, LC, N_PCOL, TILE, TILE).transpose(1, 0, 3, 2, 4, 5)
    column = grid_tiles[:, 0]
    diag_block = column[0]
    lower = jnp.linalg.cholesky(0.5 * (diag_block + diag_block.T))
    flat = column.reshape(NT * TILE, TILE)
    solved = jax.scipy.linalg.solve_triangular(lower, flat.T, lower=True)
    panel = solved.T.reshape(LR_DEV, N_PROW, TILE, TILE).transpose(1, 0, 2, 3)
    return (schur, panel)
```

```python
import functools

import jax
import jax.numpy as jnp
from jax import lax
from jax.experimental import pallas as pl
from jax.experimental.pallas import tpu as pltpu
from jax.sharding import Mesh, PartitionSpec as P

HIGHEST = lax.Precision.HIGHEST
MESH = pl.DeviceIdType.MESH


def split(x):
    high = x.astype(jnp.bfloat16)
    low = (x - high.astype(jnp.float32)).astype(jnp.bfloat16)
    return high, low


def dot3(a_high, a_low, b_high, b_low):
    dot = functools.partial(jnp.dot, preferred_element_type=jnp.float32)
    return dot(a_high, b_high) + (dot(a_high, b_low) + dot(a_low, b_high))


def members(tiles_ref, row, count, modulus, residue, want):
    found, places = [jnp.int32(0)] * want, [jnp.int32(0)] * want
    seen = jnp.int32(0)
    for j in range(count):
        tile = tiles_ref[row, j]
        match = lax.rem(tile, modulus) == residue
        for k in range(want):
            hit = match & (seen == k)
            found[k] = jnp.where(hit, tile, found[k])
            places[k] = jnp.where(hit, jnp.int32(j), places[k])
        seen = seen + match.astype(jnp.int32)
    return found, places


def factor_inverse_of(matrix):
    size = matrix.shape[0]
    rows = lax.broadcasted_iota(jnp.int32, matrix.shape, 0)
    cols = lax.broadcasted_iota(jnp.int32, matrix.shape, 1)

    def eliminate(j, carry):
        rest, inverse = carry
        row = jnp.sum(jnp.where(rows == j, rest, 0.0), axis=0, keepdims=True)
        column = jnp.sum(jnp.where(cols == j, rest, 0.0), axis=1, keepdims=True)
        pivot = jnp.sum(jnp.where(cols[:1] == j, row, 0.0), axis=1, keepdims=True)
        scale = 1.0 / jnp.sqrt(pivot)
        below = jnp.where(rows[:, :1] > j, column * scale, 0.0)
        solved = jnp.sum(jnp.where(rows == j, inverse, 0.0), axis=0, keepdims=True) * scale
        rest = rest - below * (row * scale)
        inverse = jnp.where(rows == j, solved, inverse - below * solved)
        return rest, inverse

    return lax.fori_loop(0, size, eliminate, (matrix, (rows == cols).astype(jnp.float32)))[1]


def exchange_kernel(
    halves, half_rows, cols_grid, rows_per, local_cols, width,
    tiles_ref, sizes_ref, coupling_ref, factor_ref, base_ref,
    own_ref, far_ref, inverse_ref, slots_ref,
    block_ref, square_ref, corner_ref, w_ref, across_ref, high_ref, low_ref, stage_ref, sums_ref, heard_ref,
    load_sem, across_send, across_recv, own_send, own_recv, far_send, far_recv, local_sem, sum_send, sum_recv,
):
    rows_grid = halves * half_rows
    group = half_rows * cols_grid
    laps = rows_grid // cols_grid
    iface = coupling_ref.shape[1]
    tile_count = iface // width
    block = rows_per * width
    half, sub, pcol = lax.axis_index("half"), lax.axis_index("sub"), lax.axis_index("pcol")
    prow = half * half_rows + sub
    me = sub * cols_grid + pcol
    self_index = half * group + me
    opposite = lax.rem(half + 1, halves)

    loads = [
        pltpu.make_async_copy(factor_ref, square_ref, load_sem.at[0]),
        pltpu.make_async_copy(base_ref.at[0], corner_ref, load_sem.at[1]),
    ]
    for j in range(tile_count):
        tile = coupling_ref.at[:, j * width : (j + 1) * width]
        loads.append(pltpu.make_async_copy(tile, block_ref.at[j], load_sem.at[2 + j]))
    for load in loads:
        load.start()

    def place(peer):
        return (half, peer // cols_grid, lax.rem(peer, cols_grid))

    barrier = pltpu.get_barrier_semaphore()

    def greet(k, carry):
        pl.semaphore_signal(barrier, inc=1, device_id=place(lax.rem(me + k, group)), device_id_type=MESH)
        return carry

    lax.fori_loop(1, group, greet, 0)
    pl.semaphore_signal(barrier, inc=1, device_id=(opposite, sub, pcol), device_id_type=MESH)

    order = []
    for m in range(rows_grid):
        order += members(tiles_ref, self_index, tile_count, rows_grid, m, rows_per)[1]
    first = jnp.int32(0)
    present = jnp.int32(0)
    for j in range(tile_count):
        hit = tiles_ref[self_index, j] == 0
        first = jnp.where(hit, jnp.int32(j), first)
        present = jnp.where(hit, jnp.int32(1), present)

    for load in loads:
        load.wait()
    factor_high, factor_low = split(square_ref[...])
    size = sizes_ref[0]

    def weigh(columns, limit):
        live = lax.broadcasted_iota(jnp.int32, columns.shape, 0) < limit
        product = dot3(factor_high, factor_low, *split(jnp.where(live, columns, 0.0)))
        return jnp.where(live, product, 0.0)

    product = weigh(block_ref[first], size * present)
    square = dot3(*split(product.T), *split(product))
    sums_ref[0] = jnp.where(self_index == 0, corner_ref[...], 0.0) - square

    def across_copy(m):
        return pltpu.make_async_remote_copy(
            src_ref=w_ref.at[m],
            dst_ref=across_ref.at[m],
            send_sem=across_send.at[m],
            recv_sem=across_recv.at[m],
            device_id=(opposite, sub, pcol),
            device_id_type=MESH,
        )

    for m in range(rows_grid):
        columns = jnp.concatenate([block_ref[at] for at in order[m * rows_per : (m + 1) * rows_per]], axis=1)
        product = weigh(columns, size)
        w_ref[m] = product
        high, low = split(product)
        high_ref[m] = high
        low_ref[m] = low
        if m == 0:
            pl.semaphore_wait(barrier, group)
        across_copy(m).start()

    def spread(source_ref, out_ref, send_sem, recv_sem):
        def copy_to(peer):
            return pltpu.make_async_remote_copy(
                src_ref=stage_ref.at[peer],
                dst_ref=out_ref.at[me],
                send_sem=send_sem.at[peer],
                recv_sem=recv_sem.at[me],
                device_id=place(peer),
                device_id_type=MESH,
            )

        def arriving(peer):
            return pltpu.make_async_remote_copy(
                src_ref=stage_ref.at[peer],
                dst_ref=out_ref.at[peer],
                send_sem=send_sem.at[peer],
                recv_sem=recv_sem.at[peer],
                device_id=place(peer),
                device_id_type=MESH,
            )

        def step(i, carry):
            target = lax.rem(sub + 1 + i, half_rows)
            row_high, row_low = split(source_ref[half * half_rows + target].T)
            for m in range(rows_grid):
                q, lap = m % cols_grid, m // cols_grid
                product = dot3(row_high, row_low, high_ref[m], low_ref[m])
                for r in range(rows_per):
                    for c in range(rows_per):
                        stage_ref[target * cols_grid + q, r, lap * rows_per + c] = product[
                            r * width : (r + 1) * width, c * width : (c + 1) * width
                        ]
            for shift in range(cols_grid):
                peer = target * cols_grid + lax.rem(pcol + shift, cols_grid)

                @pl.when(peer != me)
                def _():
                    copy_to(peer).start()

                @pl.when(peer == me)
                def _():
                    pltpu.make_async_copy(stage_ref.at[peer], out_ref.at[me], local_sem).start()

            return carry

        lax.fori_loop(0, half_rows, step, 0)

        def sent():
            pltpu.make_async_copy(stage_ref.at[me], out_ref.at[me], local_sem).wait()

            def wait(k, carry):
                copy_to(lax.rem(me + k, group)).wait_send()
                return carry

            lax.fori_loop(1, group, wait, 0)

        def arrived():
            def wait(k, carry):
                arriving(lax.rem(me + k, group)).wait_recv()
                return carry

            lax.fori_loop(1, group, wait, 0)

        return sent, arrived

    own_sent, own_arrived = spread(w_ref, own_ref, own_send, own_recv)

    steps = sums_ref.shape[0] - 1
    for k in range(steps):
        stride = 1 << (steps - 1 - k)
        peer = self_index ^ stride
        copy = pltpu.make_async_remote_copy(
            src_ref=sums_ref.at[k],
            dst_ref=heard_ref.at[k],
            send_sem=sum_send.at[k],
            recv_sem=sum_recv.at[k],
            device_id=(peer // group, lax.rem(peer, group) // cols_grid, lax.rem(peer, cols_grid)),
            device_id_type=MESH,
        )
        copy.start()
        copy.wait()
        sums_ref[k + 1] = sums_ref[k] + heard_ref[k]
    total = sums_ref[steps]
    inverse_ref[...] = factor_inverse_of(0.5 * (total + total.T))

    each = rows_per * laps * rows_per

    def place_tiles(n, carry):
        from_half = n // group
        sender = lax.rem(half + from_half, halves) * group + lax.rem(n, group)
        row_tiles = members(tiles_ref, sender, tile_count, rows_grid, prow, rows_per)[0]
        col_tiles = []
        for lap in range(laps):
            col_tiles += members(tiles_ref, sender, tile_count, rows_grid, lap * cols_grid + pcol, rows_per)[0]
        for r in range(rows_per):
            for c in range(laps * rows_per):
                slots_ref[n * each + r * laps * rows_per + c] = (
                    row_tiles[r] // rows_grid * local_cols
                    + col_tiles[c] // cols_grid
                )
        return carry

    lax.fori_loop(0, halves * group, place_tiles, 0)

    own_sent()
    for m in range(rows_grid):
        across_copy(m).wait()
        high, low = split(across_ref[m])
        high_ref[m] = high
        low_ref[m] = low
    far_sent, far_arrived = spread(across_ref, far_ref, far_send, far_recv)
    own_arrived()
    far_arrived()
    far_sent()


def exchange(tiles, sizes, coupling, factor, base, halves, half_rows, cols_grid, local_cols):
    interior, iface = coupling.shape
    width = base.shape[-1]
    rows_grid = halves * half_rows
    rows_per = iface // width // rows_grid
    cols_per = iface // width // cols_grid
    group = half_rows * cols_grid
    parts = (group, rows_per, cols_per, width, width)
    chunks = (rows_grid, interior, rows_per * width)
    steps = (halves * group).bit_length() - 1
    dma = pltpu.SemaphoreType.DMA
    anywhere = pl.BlockSpec(memory_space=pl.ANY)
    scalars = pl.BlockSpec(memory_space=pltpu.SMEM)
    return pl.pallas_call(
        functools.partial(exchange_kernel, halves, half_rows, cols_grid, rows_per, local_cols, width),
        in_specs=[scalars, scalars, anywhere, anywhere, anywhere],
        out_specs=[anywhere, anywhere, pl.BlockSpec(memory_space=pltpu.VMEM), scalars],
        out_shape=[
            jax.ShapeDtypeStruct(parts, jnp.float32),
            jax.ShapeDtypeStruct(parts, jnp.float32),
            jax.ShapeDtypeStruct((width, width), jnp.float32),
            jax.ShapeDtypeStruct((halves * group * rows_per * cols_per,), jnp.int32),
        ],
        scratch_shapes=[
            pltpu.VMEM((iface // width, interior, width), jnp.float32),
            pltpu.VMEM((interior, interior), jnp.float32),
            pltpu.VMEM((width, width), jnp.float32),
            pltpu.VMEM(chunks, jnp.float32),
            pltpu.VMEM(chunks, jnp.float32),
            pltpu.VMEM(chunks, jnp.bfloat16),
            pltpu.VMEM(chunks, jnp.bfloat16),
            pltpu.VMEM(parts, jnp.float32),
            pltpu.VMEM((steps + 1, width, width), jnp.float32),
            pltpu.VMEM((steps, width, width), jnp.float32),
            dma((iface // width + 2,)),
            dma((rows_grid,)), dma((rows_grid,)),
            dma((group,)), dma((group,)),
            dma((group,)), dma((group,)),
            dma,
            dma((steps,)), dma((steps,)),
        ],
        compiler_params=pltpu.CompilerParams(
            vmem_limit_bytes=40 << 20, collective_id=0, has_side_effects=True
        ),
        name="exchange",
    )(tiles, sizes, coupling, factor, base)


def subtract_kernel(slots_ref, base_ref, own_ref, far_ref, out_ref, sum_ref, load_sem, store_sem):
    load = pltpu.make_async_copy(base_ref, sum_ref, load_sem)
    load.start()
    load.wait()
    senders, count = own_ref.shape[:2]
    for shift, parts_ref in enumerate((own_ref, far_ref)):

        def take(n, carry):
            for i in range(count):
                slot = slots_ref[(shift * senders + n) * count + i]
                sum_ref[slot] = sum_ref[slot] - parts_ref[n, i]
            return carry

        lax.fori_loop(0, senders, take, 0)
    store = pltpu.make_async_copy(sum_ref, out_ref, store_sem)
    store.start()
    store.wait()


def subtract(slots, base, own, far):
    vmem = pl.BlockSpec(memory_space=pltpu.VMEM)
    anywhere = pl.BlockSpec(memory_space=pl.ANY)
    return pl.pallas_call(
        subtract_kernel,
        in_specs=[pl.BlockSpec(memory_space=pltpu.SMEM), anywhere, vmem, vmem],
        out_specs=anywhere,
        out_shape=jax.ShapeDtypeStruct(base.shape, jnp.float32),
        scratch_shapes=[
            pltpu.VMEM(base.shape, jnp.float32),
            pltpu.SemaphoreType.DMA,
            pltpu.SemaphoreType.DMA,
        ],
        compiler_params=pltpu.CompilerParams(vmem_limit_bytes=44 << 20),
        cost_estimate=pl.CostEstimate(
            flops=own.size + far.size, bytes_accessed=8 * own.size + 8 * base.size, transcendentals=0
        ),
        name="subtract",
    )(slots, base, own, far)


def shards(iface_tiles, interior_sizes, coupling, factor_inverse, interface_block):
    halves, half_rows = lax.axis_size("half"), lax.axis_size("sub")
    cols_grid = lax.axis_size("pcol")
    pcol_index = lax.axis_index("pcol")
    width = interface_block.shape[-1]
    local_rows, local_cols = interface_block.shape[1], interface_block.shape[3]
    share = width // cols_grid
    group = half_rows * cols_grid

    base = interface_block.reshape(local_rows * local_cols, width, width)
    own, far, inverse, slots = exchange(
        iface_tiles, interior_sizes, coupling[0], factor_inverse[0], base, halves, half_rows, cols_grid, local_cols
    )
    summed = subtract(
        slots, base, own.reshape(group, -1, width, width), far.reshape(group, -1, width, width)
    )
    schur = summed.reshape(interface_block.shape)

    column = summed.reshape(local_rows, local_cols, width, width)[:, 0]
    kept = jnp.where(pcol_index == 0, column[:, :share], 0.0)
    for q in range(1, cols_grid):
        kept = kept + lax.ppermute(column[:, q * share : (q + 1) * share], "pcol", [(0, q)])
    panel = jnp.einsum("atu,vu->atv", kept, inverse, precision=HIGHEST)
    return (schur, panel[None])


def solution(mesh):
    rows_grid, cols_grid = mesh.shape["prow"], mesh.shape["pcol"]
    grid = Mesh(
        mesh.devices.reshape(2, rows_grid // 2, cols_grid), ("half", "sub", "pcol")
    )
    prow = ("half", "sub")
    every = ("half", "sub", "pcol")
    in_specs = (
        P(),
        P(every),
        P(every, None, None),
        P(every, None, None),
        P(prow, None, "pcol", None, None, None),
    )
    out_specs = (P(prow, None, "pcol", None, None, None), P(prow, None, "pcol", None))
    return jax.shard_map(shards, mesh=grid, in_specs=in_specs, out_specs=out_specs, check_vma=False)
```

```python
import functools

import jax
import jax.numpy as jnp
from jax import lax
from jax.experimental import pallas as pl
from jax.experimental.pallas import tpu as pltpu
from jax.sharding import Mesh, PartitionSpec as P

HIGHEST = lax.Precision.HIGHEST
MESH = pl.DeviceIdType.MESH
LAYERS = 4


def split(x):
    high = x.astype(jnp.bfloat16)
    low = (x - high.astype(jnp.float32)).astype(jnp.bfloat16)
    return high, low


def dot3(a_high, a_low, b_high, b_low):
    dot = functools.partial(jnp.dot, preferred_element_type=jnp.float32)
    return dot(a_high, b_high) + (dot(a_high, b_low) + dot(a_low, b_high))


def members(tiles_ref, row, count, modulus, residue, want):
    found, places = [jnp.int32(0)] * want, [jnp.int32(0)] * want
    seen = jnp.int32(0)
    for j in range(count):
        tile = tiles_ref[row, j]
        match = lax.rem(tile, modulus) == residue
        for k in range(want):
            hit = match & (seen == k)
            found[k] = jnp.where(hit, tile, found[k])
            places[k] = jnp.where(hit, jnp.int32(j), places[k])
        seen = seen + match.astype(jnp.int32)
    return found, places


def factor_inverse_of(matrix):
    size = matrix.shape[0]
    rows = lax.broadcasted_iota(jnp.int32, matrix.shape, 0)
    cols = lax.broadcasted_iota(jnp.int32, matrix.shape, 1)

    def eliminate(j, carry):
        rest, inverse = carry
        row = jnp.sum(jnp.where(rows == j, rest, 0.0), axis=0, keepdims=True)
        column = jnp.sum(jnp.where(cols == j, rest, 0.0), axis=1, keepdims=True)
        pivot = jnp.sum(jnp.where(cols[:1] == j, row, 0.0), axis=1, keepdims=True)
        scale = 1.0 / jnp.sqrt(pivot)
        below = jnp.where(rows[:, :1] > j, column * scale, 0.0)
        solved = jnp.sum(jnp.where(rows == j, inverse, 0.0), axis=0, keepdims=True) * scale
        rest = rest - below * (row * scale)
        inverse = jnp.where(rows == j, solved, inverse - below * solved)
        return rest, inverse

    return lax.fori_loop(0, size, eliminate, (matrix, (rows == cols).astype(jnp.float32)))[1]


def exchange_kernel(
    layers, layer_rows, cols_grid, rows_per, local_cols, width,
    tiles_ref, sizes_ref, coupling_ref, factor_ref, base_ref,
    parts_ref, start_ref, inverse_ref, slots_ref,
    block_ref, square_ref, corner_ref, w_ref, high_ref, low_ref, row_high_ref, row_low_ref, stage_ref, sums_ref, heard_ref,
    load_sem, base_sem, up_send, down_send, arrive, tile_send, tile_recv, sum_send, sum_recv,
):
    classes = layers * layer_rows
    group = layer_rows * cols_grid
    laps = classes // cols_grid
    tile_count = block_ref.shape[0]
    layer, sub, pcol = lax.axis_index("layer"), lax.axis_index("sub"), lax.axis_index("pcol")
    me = sub * cols_grid + pcol
    self_index = layer * group + me
    prow = layer * layer_rows + sub
    last = layers - 1

    loads = [
        pltpu.make_async_copy(factor_ref, square_ref, load_sem.at[0]),
        pltpu.make_async_copy(base_ref.at[0], corner_ref, load_sem.at[1]),
    ]
    for j in range(tile_count):
        tile = coupling_ref.at[:, j * width : (j + 1) * width]
        loads.append(pltpu.make_async_copy(tile, block_ref.at[j], load_sem.at[2 + j]))
    for load in loads:
        load.start()
    preload = pltpu.make_async_copy(base_ref, start_ref, base_sem)
    preload.start()

    barrier = pltpu.get_barrier_semaphore()

    def greet(k, carry):
        peer = lax.rem(me + k, group)
        pl.semaphore_signal(
            barrier, inc=1, device_id=(layer, peer // cols_grid, lax.rem(peer, cols_grid)), device_id_type=MESH
        )
        return carry

    lax.fori_loop(1, group, greet, 0)
    for other in (last - layer, layer ^ 1):
        pl.semaphore_signal(barrier, inc=1, device_id=(other, sub, pcol), device_id_type=MESH)

    first = jnp.int32(0)
    present = jnp.int32(0)
    for j in range(tile_count):
        hit = tiles_ref[self_index, j] == 0
        first = jnp.where(hit, jnp.int32(j), first)
        present = jnp.where(hit, jnp.int32(1), present)

    for load in loads:
        load.wait()
    factor_high, factor_low = split(square_ref[...])
    size = sizes_ref[0]

    def weigh(columns, limit):
        live = lax.broadcasted_iota(jnp.int32, columns.shape, 0) < limit
        product = dot3(factor_high, factor_low, *split(jnp.where(live, columns, 0.0)))
        return jnp.where(live, product, 0.0)

    product = weigh(block_ref[first], size * present)
    square = dot3(*split(product.T), *split(product))
    sums_ref[0] = jnp.where(self_index == 0, corner_ref[...], 0.0) - square

    def up_copy(source, m):
        return pltpu.make_async_remote_copy(
            src_ref=w_ref.at[source, m],
            dst_ref=w_ref.at[source, m],
            send_sem=up_send.at[source, m],
            recv_sem=arrive.at[source, m],
            device_id=(jnp.minimum(layer + 1, last), sub, pcol),
            device_id_type=MESH,
        )

    def down_copy(source, m):
        return pltpu.make_async_remote_copy(
            src_ref=w_ref.at[source, m],
            dst_ref=w_ref.at[source, m],
            send_sem=down_send.at[source, m],
            recv_sem=arrive.at[source, m],
            device_id=(jnp.maximum(layer - 1, 0), sub, pcol),
            device_id_type=MESH,
        )

    def pass_up(source, m):
        @pl.when(layer < last)
        def _():
            up_copy(source, m).start()

    def pass_down(source, m):
        @pl.when(layer > 0)
        def _():
            down_copy(source, m).start()

    steps = sums_ref.shape[0] - 1

    def sum_copy(k):
        if k == 0:
            partner = (last - layer, sub, pcol)
        elif k == 1:
            partner = (layer ^ 1, sub, pcol)
        else:
            peer = me ^ (group >> (k - 1))
            partner = (layer, peer // cols_grid, lax.rem(peer, cols_grid))
        return pltpu.make_async_remote_copy(
            src_ref=sums_ref.at[k],
            dst_ref=heard_ref.at[k],
            send_sem=sum_send.at[k],
            recv_sem=sum_recv.at[k],
            device_id=partner,
            device_id_type=MESH,
        )

    def sum_up(k):
        sum_copy(k).wait()
        sums_ref[k + 1] = sums_ref[k] + heard_ref[k]

    def keep(m, product):
        high, low = split(product)
        high_ref[m] = high
        low_ref[m] = low

    def weigh_class(m):
        order = members(tiles_ref, self_index, tile_count, classes, m, rows_per)[1]
        product = weigh(jnp.concatenate([block_ref[at] for at in order], axis=1), size)
        w_ref[layer, m] = product
        keep(m, product)

    pl.semaphore_wait(barrier, group + 1)
    sum_copy(0).start()
    weigh_class(0)
    sum_up(0)
    sum_copy(1).start()
    weigh_class(last * layer_rows)
    sum_up(1)
    sum_copy(2).start()
    for m in (0, last * layer_rows):
        pass_up(layer, m)
        pass_down(layer, m)

    def weigh_rest(m, carry):
        @pl.when((m != 0) & (m != last * layer_rows))
        def _():
            weigh_class(m)
            pass_up(layer, m)
            pass_down(layer, m)

        return carry

    lax.fori_loop(0, classes, weigh_rest, 0)
    for k in range(2, steps):
        sum_up(k)
        if k + 1 < steps:
            sum_copy(k + 1).start()

    def tiles_out(source, m, slot, target):
        q, lap = lax.rem(m, cols_grid), m // cols_grid
        return pltpu.make_async_remote_copy(
            src_ref=stage_ref.at[slot, m, target],
            dst_ref=parts_ref.at[source * group + me, lap],
            send_sem=tile_send.at[slot, m, target],
            recv_sem=tile_recv.at[source * group + me, lap],
            device_id=(layer, target, q),
            device_id_type=MESH,
        )

    def take_rows(source):
        for t in range(layer_rows):
            high, low = split(w_ref[source, layer * layer_rows + t].T)
            row_high_ref[t] = high
            row_low_ref[t] = low

    def column(source, m, slot):
        q, lap = lax.rem(m, cols_grid), m // cols_grid
        for t in range(layer_rows):
            product = dot3(row_high_ref[t], row_low_ref[t], high_ref[m], low_ref[m])
            away = (q != pcol) | (sub != t)

            def write(ref):
                for r in range(rows_per):
                    for c in range(rows_per):
                        ref[r, c] = product[r * width : (r + 1) * width, c * width : (c + 1) * width]

            @pl.when(away)
            def _():
                write(stage_ref.at[slot, m, t])
                tiles_out(source, m, slot, t).start()

            @pl.when(jnp.logical_not(away))
            def _():
                write(parts_ref.at[source * group + me, lap])

    def sent(source, slot):
        def wait(n, carry):
            m, t = n // layer_rows, lax.rem(n, layer_rows)

            @pl.when((lax.rem(m, cols_grid) != pcol) | (sub != t))
            def _():
                tiles_out(source, m, slot, t).wait_send()

            return carry

        lax.fori_loop(0, classes * layer_rows, wait, 0)

    def columns(source, slot, ordered, low, top):
        def step(i, carry):
            column(source, ordered(i), slot)
            return carry

        lax.fori_loop(low, top, step, 0)

    def straight(i):
        return i

    middle = classes // 2

    def up_order(i):
        near_end = classes - layer_rows * (1 + i // layer_rows) + lax.rem(i, layer_rows)
        return jnp.where(i < middle, near_end, lax.rem(i + 1 + pcol, middle))

    def down_order(i):
        return jnp.where(i < middle, i, middle + lax.rem(i + 1 + pcol, middle))

    take_rows(layer)
    columns(layer, 0, straight, 0, classes)

    total = sums_ref[steps]
    inverse_ref[...] = factor_inverse_of(0.5 * (total + total.T))

    each = rows_per * laps * rows_per

    def place_tiles(sender, carry):
        row_tiles = members(tiles_ref, sender, tile_count, classes, prow, rows_per)[0]
        for lap in range(laps):
            col_tiles = members(tiles_ref, sender, tile_count, classes, lap * cols_grid + pcol, rows_per)[0]
            for r in range(rows_per):
                for c in range(rows_per):
                    slots_ref[sender * each + (lap * rows_per + r) * rows_per + c] = (
                        row_tiles[r] // classes * local_cols + col_tiles[c] // cols_grid
                    )
        return carry

    def relay(i, carry):
        @pl.when(layer > 0)
        def _():
            source, m = layer - 1, up_order(i)
            up_copy(source, m).wait_recv()
            pass_up(source, m)

        @pl.when(layer < last)
        def _():
            source, m = layer + 1, down_order(i)
            down_copy(source, m).wait_recv()
            pass_down(source, m)

        return carry

    lax.fori_loop(0, classes, relay, 0)

    def absorb(source, slot):
        def prepare(m, carry):
            keep(m, w_ref[source, m])
            return carry

        lax.fori_loop(0, classes, prepare, 0)
        take_rows(source)
        columns(source, slot, straight, 0, classes)

    @pl.when(layer > 0)
    def _():
        absorb(layer - 1, 1)

    sent(layer, 0)

    @pl.when(layer < last)
    def _():
        absorb(layer + 1, 0)

    @pl.when(layer > 0)
    def _():
        sent(layer - 1, 1)

    rising = layer >= layers // 2

    def order(i):
        return jnp.where(rising, up_order(i), down_order(i))

    def stream(distance, slot, passing):
        source = jnp.where(rising, layer - distance, layer + distance)

        def receive(i):
            m = order(i)
            up_copy(source, m).wait_recv()
            if passing:

                @pl.when(rising)
                def _():
                    pass_up(source, m)

                @pl.when(jnp.logical_not(rising))
                def _():
                    pass_down(source, m)

            keep(m, w_ref[source, m])
            return m

        def gather(i, carry):
            receive(i)
            return carry

        lax.fori_loop(0, middle, gather, 0)
        take_rows(source)
        columns(source, slot, order, 0, middle)

        def step(i, carry):
            column(source, receive(i), slot)
            return carry

        lax.fori_loop(middle, classes, step, 0)

    stream(2, 1, True)
    lax.fori_loop(0, layers * group, place_tiles, 0)

    @pl.when(layer < last)
    def _():
        sent(layer + 1, 0)

    ends = (layer == 0) | (layer == last)

    @pl.when(ends)
    def _():
        stream(3, 0, False)

    def landed(n, carry):
        source, k = n // group, lax.rem(n, group)

        @pl.when(k > 0)
        def _():
            peer = lax.rem(me + k, group)
            for lap in range(laps):
                pltpu.make_async_remote_copy(
                    src_ref=stage_ref.at[0, 0, 0],
                    dst_ref=parts_ref.at[source * group + peer, lap],
                    send_sem=tile_send.at[0, 0, 0],
                    recv_sem=tile_recv.at[source * group + peer, lap],
                    device_id=(layer, peer // cols_grid, lax.rem(peer, cols_grid)),
                    device_id_type=MESH,
                ).wait_recv()

        return carry

    lax.fori_loop(0, layers * group, landed, 0)
    sent(jnp.where(rising, layer - 2, layer + 2), 1)

    @pl.when(ends)
    def _():
        sent(jnp.where(rising, layer - 3, layer + 3), 0)

    def passed(source, carry):
        def wait(m, inner):
            @pl.when((source <= layer) & (layer < last))
            def _():
                up_copy(source, m).wait_send()

            @pl.when((source >= layer) & (layer > 0))
            def _():
                down_copy(source, m).wait_send()

            return inner

        return lax.fori_loop(0, classes, wait, carry)

    lax.fori_loop(0, layers, passed, 0)
    preload.wait()


def exchange(tiles, sizes, coupling, factor, base, layers, layer_rows, cols_grid, local_cols):
    interior, iface = coupling.shape
    width = base.shape[-1]
    classes = layers * layer_rows
    rows_per = iface // width // classes
    laps = classes // cols_grid
    group = layer_rows * cols_grid
    senders = layers * group
    parts = (senders, laps, rows_per, rows_per, width, width)
    chunks = (classes, interior, rows_per * width)
    steps = senders.bit_length() - 1
    dma = pltpu.SemaphoreType.DMA
    vmem = pl.BlockSpec(memory_space=pltpu.VMEM)
    hbm = pl.BlockSpec(memory_space=pltpu.HBM)
    scalars = pl.BlockSpec(memory_space=pltpu.SMEM)
    return pl.pallas_call(
        functools.partial(exchange_kernel, layers, layer_rows, cols_grid, rows_per, local_cols, width),
        in_specs=[scalars, scalars, hbm, hbm, hbm],
        out_specs=[vmem, vmem, vmem, scalars],
        out_shape=[
            pltpu.VMEM(parts, jnp.float32),
            pltpu.VMEM(base.shape, jnp.float32),
            jax.ShapeDtypeStruct((width, width), jnp.float32),
            jax.ShapeDtypeStruct((senders * laps * rows_per * rows_per,), jnp.int32),
        ],
        scratch_shapes=[
            pltpu.VMEM((iface // width, interior, width), jnp.float32),
            pltpu.VMEM((interior, interior), jnp.float32),
            pltpu.VMEM((width, width), jnp.float32),
            pltpu.VMEM((layers, *chunks), jnp.float32),
            pltpu.VMEM(chunks, jnp.bfloat16),
            pltpu.VMEM(chunks, jnp.bfloat16),
            pltpu.VMEM((layer_rows, rows_per * width, interior), jnp.bfloat16),
            pltpu.VMEM((layer_rows, rows_per * width, interior), jnp.bfloat16),
            pltpu.VMEM((2, classes, layer_rows, rows_per, rows_per, width, width), jnp.float32),
            pltpu.VMEM((steps + 1, width, width), jnp.float32),
            pltpu.VMEM((steps, width, width), jnp.float32),
            dma((iface // width + 2,)), dma,
            dma((layers, classes)), dma((layers, classes)), dma((layers, classes)),
            dma((2, classes, layer_rows)), dma((senders, laps)),
            dma((steps,)), dma((steps,)),
        ],
        compiler_params=pltpu.CompilerParams(
            vmem_limit_bytes=38 << 20, collective_id=0, has_side_effects=True
        ),
        name="exchange",
    )(tiles, sizes, *(pltpu.with_memory_space_constraint(x, pltpu.HBM) for x in (coupling, factor, base)))


def subtract_kernel(slots_ref, start_ref, parts_ref, out_ref, sum_ref, store_sem):
    senders, count = parts_ref.shape[:2]

    def take(n, carry):
        for i in range(count):
            slot = slots_ref[n * count + i]
            sum_ref[slot] = sum_ref[slot] - parts_ref[n, i]
        return carry

    lax.fori_loop(0, senders, take, 0)
    store = pltpu.make_async_copy(sum_ref, out_ref, store_sem)
    store.start()
    store.wait()


def subtract(slots, start, parts):
    vmem = pl.BlockSpec(memory_space=pltpu.VMEM)
    return pl.pallas_call(
        subtract_kernel,
        in_specs=[pl.BlockSpec(memory_space=pltpu.SMEM), vmem, vmem],
        out_specs=[pl.BlockSpec(memory_space=pltpu.HBM), vmem],
        out_shape=[pltpu.HBM(start.shape, jnp.float32), pltpu.VMEM(start.shape, jnp.float32)],
        input_output_aliases={1: 1},
        scratch_shapes=[pltpu.SemaphoreType.DMA],
        compiler_params=pltpu.CompilerParams(vmem_limit_bytes=1 << 20),
        cost_estimate=pl.CostEstimate(
            flops=parts.size, bytes_accessed=8 * parts.size + 4 * start.size, transcendentals=0
        ),
        name="subtract",
    )(slots, start, parts)


def shards(iface_tiles, interior_sizes, coupling, factor_inverse, interface_block):
    layers, layer_rows = lax.axis_size("layer"), lax.axis_size("sub")
    cols_grid = lax.axis_size("pcol")
    pcol_index = lax.axis_index("pcol")
    width = interface_block.shape[-1]
    local_rows, local_cols = interface_block.shape[1], interface_block.shape[3]
    share = width // cols_grid

    base = interface_block.reshape(local_rows * local_cols, width, width)
    parts, start, inverse, slots = exchange(
        iface_tiles, interior_sizes, coupling[0], factor_inverse[0], base, layers, layer_rows, cols_grid, local_cols
    )
    summed, kept_tiles = subtract(slots, start, parts.reshape(parts.shape[0], -1, width, width))
    schur = summed.reshape(interface_block.shape)

    column = kept_tiles.reshape(local_rows, local_cols, width, width)[:, 0]
    kept = jnp.where(pcol_index == 0, column[:, :share], 0.0)
    for q in range(1, cols_grid):
        kept = kept + lax.ppermute(column[:, q * share : (q + 1) * share], "pcol", [(0, q)])
    panel = jnp.einsum("atu,vu->atv", kept, inverse, precision=HIGHEST)
    return (schur, panel[None])


def solution(mesh):
    rows_grid, cols_grid = mesh.shape["prow"], mesh.shape["pcol"]
    grid = Mesh(
        mesh.devices.reshape(LAYERS, rows_grid // LAYERS, cols_grid), ("layer", "sub", "pcol")
    )
    prow = ("layer", "sub")
    every = ("layer", "sub", "pcol")
    in_specs = (
        P(),
        P(every),
        P(every, None, None),
        P(every, None, None),
        P(prow, None, "pcol", None, None, None),
    )
    out_specs = (P(prow, None, "pcol", None, None, None), P(prow, None, "pcol", None))
    return jax.shard_map(shards, mesh=grid, in_specs=in_specs, out_specs=out_specs, check_vma=False)
```

```python
import functools

import jax
import jax.numpy as jnp
from jax import lax
from jax.experimental import pallas as pl
from jax.experimental.pallas import tpu as pltpu
from jax.sharding import Mesh, PartitionSpec as P

HIGHEST = lax.Precision.HIGHEST
MESH = pl.DeviceIdType.MESH
LAYERS = 4


def split(x):
    high = x.astype(jnp.bfloat16)
    low = (x - high.astype(jnp.float32)).astype(jnp.bfloat16)
    return high, low


def dot3(a_high, a_low, b_high, b_low):
    dot = functools.partial(jnp.dot, preferred_element_type=jnp.float32)
    return dot(a_high, b_high) + (dot(a_high, b_low) + dot(a_low, b_high))


def members(tiles_ref, row, count, modulus, residue, want):
    found, places = [jnp.int32(0)] * want, [jnp.int32(0)] * want
    seen = jnp.int32(0)
    for j in range(count):
        tile = tiles_ref[j, row]
        match = lax.rem(tile, modulus) == residue
        for k in range(want):
            hit = match & (seen == k)
            found[k] = jnp.where(hit, tile, found[k])
            places[k] = jnp.where(hit, jnp.int32(j), places[k])
        seen = seen + match.astype(jnp.int32)
    return found, places


def factor_inverse_of(matrix):
    size = matrix.shape[0]
    rows = lax.broadcasted_iota(jnp.int32, matrix.shape, 0)
    cols = lax.broadcasted_iota(jnp.int32, matrix.shape, 1)

    def eliminate(j, carry):
        rest, inverse = carry
        row = jnp.sum(jnp.where(rows == j, rest, 0.0), axis=0, keepdims=True)
        column = jnp.sum(jnp.where(cols == j, rest, 0.0), axis=1, keepdims=True)
        pivot = jnp.sum(jnp.where(cols[:1] == j, row, 0.0), axis=1, keepdims=True)
        scale = 1.0 / jnp.sqrt(pivot)
        below = jnp.where(rows[:, :1] > j, column * scale, 0.0)
        solved = jnp.sum(jnp.where(rows == j, inverse, 0.0), axis=0, keepdims=True) * scale
        rest = rest - below * (row * scale)
        inverse = jnp.where(rows == j, solved, inverse - below * solved)
        return rest, inverse

    return lax.fori_loop(0, size, eliminate, (matrix, (rows == cols).astype(jnp.float32)))[1]


def exchange_kernel(
    layers, layer_rows, cols_grid, rows_per, width,
    tiles_ref, sizes_ref, coupling_ref, factor_ref, base_ref,
    parts_ref, start_ref, side_ref, side_start_ref, inverse_ref, slots_ref,
    block_ref, corner_ref, w_ref, high_ref, low_ref, row_high_ref, row_low_ref, stage_ref, sums_ref, heard_ref,
    load_sem, base_sem, up_send, down_send, arrive, tile_send, tile_recv, side_send, side_recv, share_send, share_recv, sum_send, sum_recv,
):
    classes = layers * layer_rows
    group = layer_rows * cols_grid
    laps = classes // cols_grid
    tile_count = block_ref.shape[0]
    layer, sub, pcol = lax.axis_index("layer"), lax.axis_index("sub"), lax.axis_index("pcol")
    me = sub * cols_grid + pcol
    self_index = layer * group + me
    prow = layer * layer_rows + sub
    last = layers - 1
    block = rows_per * width
    local_cols = base_ref.shape[1]
    share = side_ref.shape[3]

    interior = factor_ref.shape[0]
    side = interior // width

    def factor_tile(n):
        rest, c = divmod(n, rows_per)
        rest, r = divmod(rest, rows_per)
        m, t = divmod(rest, layer_rows)
        return stage_ref.at[1, m, t, r, c]

    def spot(n):
        return slice(n // side * width, (n // side + 1) * width), slice(n % side * width, (n % side + 1) * width)

    loads = [pltpu.make_async_copy(base_ref.at[0, 0], corner_ref, load_sem.at[0])]
    for n in range(side * side):
        loads.append(pltpu.make_async_copy(factor_ref.at[spot(n)], factor_tile(n), load_sem.at[1 + n]))
    for j in range(tile_count):
        tile = coupling_ref.at[:, j * width : (j + 1) * width]
        loads.append(pltpu.make_async_copy(tile, block_ref.at[j], load_sem.at[1 + side * side + j]))
    for load in loads:
        load.start()
    preload = pltpu.make_async_copy(base_ref, start_ref, base_sem)
    preload.start()

    barrier = pltpu.get_barrier_semaphore()

    def greet(k, carry):
        peer = lax.rem(me + k, group)
        pl.semaphore_signal(
            barrier, inc=1, device_id=(layer, peer // cols_grid, lax.rem(peer, cols_grid)), device_id_type=MESH
        )
        return carry

    lax.fori_loop(1, group, greet, 0)
    for other in (last - layer, layer ^ 1):
        pl.semaphore_signal(barrier, inc=1, device_id=(other, sub, pcol), device_id_type=MESH)

    first = jnp.int32(0)
    present = jnp.int32(0)
    for j in range(tile_count):
        hit = tiles_ref[j, self_index] == 0
        first = jnp.where(hit, jnp.int32(j), first)
        present = jnp.where(hit, jnp.int32(1), present)

    for load in loads:
        load.wait()
    for n in range(side * side):
        high, low = split(factor_tile(n)[...])
        row_high_ref[spot(n)] = high
        row_low_ref[spot(n)] = low
    size = sizes_ref[0]

    def weigh(columns, limit):
        live = lax.broadcasted_iota(jnp.int32, columns.shape, 0) < limit
        product = dot3(row_high_ref[:interior], row_low_ref[:interior], *split(jnp.where(live, columns, 0.0)))
        return jnp.where(live, product, 0.0)

    def up_copy(source, m, c):
        return pltpu.make_async_remote_copy(
            src_ref=w_ref.at[source, m, :, c * width : (c + 1) * width],
            dst_ref=w_ref.at[source, m, :, c * width : (c + 1) * width],
            send_sem=up_send.at[source, m, c],
            recv_sem=arrive.at[source, m, c],
            device_id=(jnp.minimum(layer + 1, last), sub, pcol),
            device_id_type=MESH,
        )

    def down_copy(source, m, c):
        return pltpu.make_async_remote_copy(
            src_ref=w_ref.at[source, m, :, c * width : (c + 1) * width],
            dst_ref=w_ref.at[source, m, :, c * width : (c + 1) * width],
            send_sem=down_send.at[source, m, c],
            recv_sem=arrive.at[source, m, c],
            device_id=(jnp.maximum(layer - 1, 0), sub, pcol),
            device_id_type=MESH,
        )

    def pass_up(source, m):
        @pl.when(layer < last)
        def _():
            for c in range(rows_per):
                up_copy(source, m, c).start()

    def pass_down(source, m):
        @pl.when(layer > 0)
        def _():
            for c in range(rows_per):
                down_copy(source, m, c).start()

    steps = sums_ref.shape[0] - 1

    def sum_copy(k):
        if k == 0:
            partner = (last - layer, sub, pcol)
        elif k == 1:
            partner = (layer ^ 1, sub, pcol)
        else:
            peer = me ^ (group >> (k - 1))
            partner = (layer, peer // cols_grid, lax.rem(peer, cols_grid))
        return pltpu.make_async_remote_copy(
            src_ref=sums_ref.at[k],
            dst_ref=heard_ref.at[k],
            send_sem=sum_send.at[k],
            recv_sem=sum_recv.at[k],
            device_id=partner,
            device_id_type=MESH,
        )

    def sum_up(k):
        sum_copy(k).wait()
        sums_ref[k + 1] = sums_ref[k] + heard_ref[k]

    def keep(m, product):
        high, low = split(product)
        high_ref[m] = high
        low_ref[m] = low

    def weigh_class(m):
        order = members(tiles_ref, self_index, tile_count, classes, m, rows_per)[1]
        product = weigh(jnp.concatenate([block_ref[at] for at in order], axis=1), size)
        w_ref[layer, m] = product
        keep(m, product)

    def share_copy(q):
        return pltpu.make_async_remote_copy(
            src_ref=base_ref.at[:, 0, q * share : (q + 1) * share, :],
            dst_ref=side_start_ref,
            send_sem=share_send.at[q],
            recv_sem=share_recv,
            device_id=(layer, sub, q),
            device_id_type=MESH,
        )

    own_share = pltpu.make_async_copy(base_ref.at[:, 0, :share, :], side_start_ref, share_send.at[0])

    middle = classes // 2

    def up_order(i):
        near_end = classes - layer_rows * (1 + i // layer_rows) + lax.rem(i, layer_rows)
        return jnp.where(i < middle, near_end, lax.rem(i + 1 + pcol, middle))

    def down_order(i):
        return jnp.where(i < middle, i, middle + lax.rem(i + 1 + pcol, middle))

    def weigh_pair(i):
        weigh_class(up_order(i))
        weigh_class(down_order(i))

    def pass_pair(i):
        pass_up(layer, up_order(i))
        pass_down(layer, down_order(i))

    weigh_pair(0)
    pl.semaphore_wait(barrier, group + 1)
    pass_pair(0)
    product = weigh(block_ref[first], size * present)
    square = dot3(*split(product.T), *split(product))
    sums_ref[0] = jnp.where(self_index == 0, corner_ref[...], 0.0) - square

    sum_copy(0).start()

    @pl.when(pcol == 0)
    def _():
        own_share.start()
        for q in range(1, cols_grid):
            share_copy(q).start()

    weigh_pair(1)
    pass_pair(1)
    weigh_pair(2)
    sum_up(0)
    sum_copy(1).start()
    pass_pair(2)

    def weigh_rest(i, carry):
        weigh_pair(i)
        return carry

    lax.fori_loop(3, middle, weigh_rest, 0)
    sum_up(1)
    sum_copy(2).start()

    def pass_rest(i, carry):
        pass_pair(i)
        return carry

    lax.fori_loop(3, classes, pass_rest, 0)
    for k in range(2, steps):
        sum_up(k)
        if k + 1 < steps:
            sum_copy(k + 1).start()

    def tiles_out(source, m, slot, target):
        q, lap = lax.rem(m, cols_grid), m // cols_grid
        return pltpu.make_async_remote_copy(
            src_ref=stage_ref.at[slot, m, target],
            dst_ref=parts_ref.at[source * group + me, lap],
            send_sem=tile_send.at[slot, m, target],
            recv_sem=tile_recv.at[source * group + me, lap],
            device_id=(layer, target, q),
            device_id_type=MESH,
        )

    def tile_out(source, m, slot, target, c):
        q, lap = lax.rem(m, cols_grid), m // cols_grid
        return pltpu.make_async_remote_copy(
            src_ref=stage_ref.at[slot, m, target, :, c],
            dst_ref=parts_ref.at[source * group + me, lap, :, c],
            send_sem=tile_send.at[slot, m, target],
            recv_sem=tile_recv.at[source * group + me, lap],
            device_id=(layer, target, q),
            device_id_type=MESH,
        )

    def side_out(source, slot, target, p):
        return pltpu.make_async_remote_copy(
            src_ref=stage_ref.at[slot, 0, target, :, :, pl.ds(p * share, share), :],
            dst_ref=side_ref.at[source * group + me],
            send_sem=side_send.at[slot, target, p],
            recv_sem=side_recv.at[source * group + me],
            device_id=(layer, target, p),
            device_id_type=MESH,
        )

    def take_rows(source):
        for t in range(layer_rows):
            high, low = split(w_ref[source, layer * layer_rows + t].T)
            row_high_ref[t * block : (t + 1) * block] = high
            row_low_ref[t * block : (t + 1) * block] = low

    def column(source, m, slot, picked):
        q, lap = lax.rem(m, cols_grid), m // cols_grid
        span = slice(picked[0] * width, (picked[-1] + 1) * width)
        for t in range(layer_rows):
            rows = slice(t * block, (t + 1) * block)
            product = dot3(row_high_ref[rows], row_low_ref[rows], high_ref[m, :, span], low_ref[m, :, span])
            away = (q != pcol) | (sub != t)

            def write(ref):
                for r in range(rows_per):
                    for n, c in enumerate(picked):
                        ref[r, c] = product[r * width : (r + 1) * width, n * width : (n + 1) * width]

            @pl.when(away | (m == 0))
            def _():
                write(stage_ref.at[slot, m, t])

            @pl.when(away)
            def _():
                if len(picked) == rows_per:
                    tiles_out(source, m, slot, t).start()
                else:
                    for c in picked:
                        tile_out(source, m, slot, t, c).start()

            @pl.when(jnp.logical_not(away))
            def _():
                write(parts_ref.at[source * group + me, lap])

            @pl.when(m == 0)
            def _():
                for p in range(cols_grid):

                    @pl.when((p == pcol) & (sub == t))
                    def _():
                        for r in range(rows_per):
                            for n, c in enumerate(picked):
                                top = r * width + p * share
                                side_ref[source * group + me, r, c] = product[
                                    top : top + share, n * width : (n + 1) * width
                                ]

                    if picked[-1] == rows_per - 1:

                        @pl.when((p != pcol) | (sub != t))
                        def _():
                            side_out(source, slot, t, p).start()

    def sent(source, slot):
        def wait(n, carry):
            m, t = n // layer_rows, lax.rem(n, layer_rows)

            @pl.when((lax.rem(m, cols_grid) != pcol) | (sub != t))
            def _():
                tiles_out(source, m, slot, t).wait_send()

            return carry

        lax.fori_loop(0, classes * layer_rows, wait, 0)
        for t in range(layer_rows):
            for p in range(cols_grid):

                @pl.when((p != pcol) | (sub != t))
                def _():
                    side_out(source, slot, t, p).wait_send()

    def columns(source, slot, ordered, low, top):
        def step(i, carry):
            column(source, ordered(i), slot, tuple(range(rows_per)))
            return carry

        lax.fori_loop(low, top, step, 0)

    def straight(i):
        return i

    take_rows(layer)
    columns(layer, 0, straight, 0, classes)

    total = sums_ref[steps]
    inverse_ref[...] = factor_inverse_of(0.5 * (total + total.T))

    each = rows_per * laps * rows_per

    def place_tiles(sender, carry):
        row_tiles = members(tiles_ref, sender, tile_count, classes, prow, rows_per)[0]
        for lap in range(laps):
            col_tiles = members(tiles_ref, sender, tile_count, classes, lap * cols_grid + pcol, rows_per)[0]
            for r in range(rows_per):
                for c in range(rows_per):
                    slots_ref[sender * each + (lap * rows_per + r) * rows_per + c] = (
                        row_tiles[r] // classes * local_cols + col_tiles[c] // cols_grid
                    )
        zeros = members(tiles_ref, sender, tile_count, classes, 0, rows_per)[0]
        pick = jnp.int32(-1)
        for c in range(rows_per):
            pick = jnp.where(zeros[c] == 0, jnp.int32(c), pick)
        slots_ref[layers * group * each + sender] = pick
        return carry

    def up_onward(source, m, c):
        @pl.when(layer < last)
        def _():
            up_copy(source, m, c).start()

    def down_onward(source, m, c):
        @pl.when(layer > 0)
        def _():
            down_copy(source, m, c).start()

    def relay(i, carry):
        @pl.when(layer > 0)
        def _():
            source, m = layer - 1, up_order(i)
            for c in range(rows_per):
                up_copy(source, m, c).wait_recv()
                up_onward(source, m, c)

        @pl.when(layer < last)
        def _():
            source, m = layer + 1, down_order(i)
            for c in range(rows_per):
                down_copy(source, m, c).wait_recv()
                down_onward(source, m, c)

        return carry

    lax.fori_loop(0, classes, relay, 0)

    def absorb(source, slot):
        def prepare(m, carry):
            keep(m, w_ref[source, m])
            return carry

        lax.fori_loop(0, classes, prepare, 0)
        take_rows(source)
        columns(source, slot, straight, 0, classes)

    @pl.when(layer > 0)
    def _():
        absorb(layer - 1, 1)

    sent(layer, 0)

    @pl.when(layer < last)
    def _():
        absorb(layer + 1, 0)

    @pl.when(layer > 0)
    def _():
        sent(layer - 1, 1)

    rising = layer >= layers // 2

    def order(i):
        return jnp.where(rising, up_order(i), down_order(i))

    def stream(distance, slot, passing):
        source = jnp.where(rising, layer - distance, layer + distance)

        def receive(m, c):
            up_copy(source, m, c).wait_recv()
            if passing:

                @pl.when(rising)
                def _():
                    up_onward(source, m, c)

                @pl.when(jnp.logical_not(rising))
                def _():
                    down_onward(source, m, c)

            half = slice(c * width, (c + 1) * width)
            high, low = split(w_ref[source, m, :, half])
            high_ref[m, :, half] = high
            low_ref[m, :, half] = low

        def gather(i, carry):
            for c in range(rows_per):
                receive(order(i), c)
            return carry

        lax.fori_loop(0, middle, gather, 0)
        take_rows(source)
        columns(source, slot, order, 0, middle)

        def step(i, carry):
            for c in range(rows_per):
                receive(order(i), c)
                column(source, order(i), slot, (c,))
            return carry

        lax.fori_loop(middle, classes, step, 0)

    stream(2, 1, True)
    lax.fori_loop(0, layers * group, place_tiles, 0)

    @pl.when(layer < last)
    def _():
        sent(layer + 1, 0)

    ends = (layer == 0) | (layer == last)

    def landed(source):
        def wait(k, carry):
            peer = lax.rem(me + k, group)
            for lap in range(laps):
                pltpu.make_async_remote_copy(
                    src_ref=stage_ref.at[0, 0, 0],
                    dst_ref=parts_ref.at[source * group + peer, lap],
                    send_sem=tile_send.at[0, 0, 0],
                    recv_sem=tile_recv.at[source * group + peer, lap],
                    device_id=(layer, peer // cols_grid, lax.rem(peer, cols_grid)),
                    device_id_type=MESH,
                ).wait_recv()
            pltpu.make_async_remote_copy(
                src_ref=stage_ref.at[0, 0, 0, :, :, pl.ds(0, share), :],
                dst_ref=side_ref.at[source * group + peer],
                send_sem=side_send.at[0, 0, 0],
                recv_sem=side_recv.at[source * group + peer],
                device_id=(layer, peer // cols_grid, lax.rem(peer, cols_grid)),
                device_id_type=MESH,
            ).wait_recv()

            return carry

        lax.fori_loop(1, group, wait, 0)

    @pl.when(pcol == 0)
    def _():
        own_share.wait()
        for q in range(1, cols_grid):
            share_copy(q).wait_send()

    @pl.when(pcol != 0)
    def _():
        share_copy(1).wait_recv()

    farthest = jnp.where(rising, layer - 3, layer + 3)

    def landed_early(source, carry):
        @pl.when(jnp.logical_not(ends) | (source != farthest))
        def _():
            landed(source)

        return carry

    lax.fori_loop(0, layers, landed_early, 0)
    sent(jnp.where(rising, layer - 2, layer + 2), 1)
    def passed(source, carry):
        def wait(m, inner):
            @pl.when((source <= layer) & (layer < last))
            def _():
                for c in range(rows_per):
                    up_copy(source, m, c).wait_send()

            @pl.when((source >= layer) & (layer > 0))
            def _():
                for c in range(rows_per):
                    down_copy(source, m, c).wait_send()

            return inner

        return lax.fori_loop(0, classes, wait, carry)

    lax.fori_loop(0, layers, passed, 0)
    preload.wait()

    @pl.when(ends)
    def _():
        stream(3, 0, False)
        landed(farthest)
        sent(farthest, 0)


def exchange(tiles, sizes, coupling, factor, base, layers, layer_rows, cols_grid):
    interior, iface = coupling.shape
    width = base.shape[-1]
    classes = layers * layer_rows
    rows_per = iface // width // classes
    laps = classes // cols_grid
    group = layer_rows * cols_grid
    senders = layers * group
    parts = (senders, laps, rows_per, rows_per, width, width)
    chunks = (classes, interior, rows_per * width)
    steps = senders.bit_length() - 1
    share = width // cols_grid
    dma = pltpu.SemaphoreType.DMA
    vmem = pl.BlockSpec(memory_space=pltpu.VMEM)
    hbm = pl.BlockSpec(memory_space=pltpu.HBM)
    scalars = pl.BlockSpec(memory_space=pltpu.SMEM)
    return pl.pallas_call(
        functools.partial(exchange_kernel, layers, layer_rows, cols_grid, rows_per, width),
        in_specs=[scalars, scalars, hbm, hbm, hbm],
        out_specs=[vmem, vmem, vmem, vmem, vmem, scalars],
        out_shape=[
            pltpu.VMEM(parts, jnp.float32),
            pltpu.VMEM(base.shape, jnp.float32),
            pltpu.VMEM((senders, rows_per, rows_per, share, width), jnp.float32),
            pltpu.VMEM((base.shape[0], share, width), jnp.float32),
            pltpu.VMEM((width, width), jnp.float32),
            jax.ShapeDtypeStruct((senders * (laps * rows_per * rows_per + 1),), jnp.int32),
        ],
        scratch_shapes=[
            pltpu.VMEM((iface // width, interior, width), jnp.float32),
            pltpu.VMEM((width, width), jnp.float32),
            pltpu.VMEM((layers, *chunks), jnp.float32),
            pltpu.VMEM(chunks, jnp.bfloat16),
            pltpu.VMEM(chunks, jnp.bfloat16),
            pltpu.VMEM((max(interior, iface // layers), interior), jnp.bfloat16),
            pltpu.VMEM((max(interior, iface // layers), interior), jnp.bfloat16),
            pltpu.VMEM((2, classes, layer_rows, rows_per, rows_per, width, width), jnp.float32),
            pltpu.VMEM((steps + 1, width, width), jnp.float32),
            pltpu.VMEM((steps, width, width), jnp.float32),
            dma((iface // width + (interior // width) ** 2 + 1,)), dma,
            dma((layers, classes, rows_per)), dma((layers, classes, rows_per)), dma((layers, classes, rows_per)),
            dma((2, classes, layer_rows)), dma((senders, laps)),
            dma((2, layer_rows, cols_grid)), dma((senders,)),
            dma((cols_grid,)), dma,
            dma((steps,)), dma((steps,)),
        ],
        compiler_params=pltpu.CompilerParams(
            vmem_limit_bytes=37 << 20, collective_id=0, has_side_effects=True
        ),
        name="exchange",
    )(tiles, sizes, *(pltpu.with_memory_space_constraint(x, pltpu.HBM) for x in (coupling, factor, base)))


def subtract_kernel(
    slots_ref, start_ref, parts_ref, side_ref, side_start_ref, inverse_ref,
    out_ref, panel_ref, sum_ref, column_ref, store_sem,
):
    senders, count = parts_ref.shape[:2]
    local_cols, rows_per = out_ref.shape[0] // side_start_ref.shape[0], side_ref.shape[1]

    def take(n, carry):
        for i in range(count):
            slot = slots_ref[n * count + i]
            sum_ref[slot] = sum_ref[slot] - parts_ref[n, i]
        return carry

    lax.fori_loop(0, senders, take, 0)
    store = pltpu.make_async_copy(sum_ref, out_ref, store_sem.at[0])
    store.start()
    column_ref[...] = side_start_ref[...]

    def pick(n, carry):
        chosen = slots_ref[senders * count + n]

        @pl.when(chosen >= 0)
        def _():
            for r in range(rows_per):
                slot = slots_ref[n * count + r * rows_per] // local_cols
                column_ref[slot] = column_ref[slot] - side_ref[n, r, chosen]

        return carry

    lax.fori_loop(0, senders, pick, 0)
    column = column_ref[...].reshape(-1, column_ref.shape[-1])
    panel = jnp.dot(column, inverse_ref[...].T, precision=HIGHEST, preferred_element_type=jnp.float32)
    column_ref[...] = panel.reshape(column_ref.shape)
    ready = pltpu.make_async_copy(column_ref, panel_ref, store_sem.at[1])
    ready.start()
    store.wait()
    ready.wait()


def subtract(slots, start, parts, side, side_start, inverse):
    vmem = pl.BlockSpec(memory_space=pltpu.VMEM)
    hbm = pl.BlockSpec(memory_space=pltpu.HBM)
    return pl.pallas_call(
        subtract_kernel,
        in_specs=[pl.BlockSpec(memory_space=pltpu.SMEM), vmem, vmem, vmem, vmem, vmem],
        out_specs=[hbm, hbm, vmem],
        out_shape=[
            pltpu.HBM(start.shape, jnp.float32),
            pltpu.HBM(side_start.shape, jnp.float32),
            pltpu.VMEM(start.shape, jnp.float32),
        ],
        input_output_aliases={1: 2},
        scratch_shapes=[pltpu.VMEM(side_start.shape, jnp.float32), pltpu.SemaphoreType.DMA((2,))],
        compiler_params=pltpu.CompilerParams(vmem_limit_bytes=2 << 20),
        cost_estimate=pl.CostEstimate(
            flops=parts.size, bytes_accessed=8 * parts.size + 4 * start.size, transcendentals=0
        ),
        name="subtract",
    )(slots, start, parts, side, side_start, inverse)


def shards(iface_tiles, interior_sizes, coupling, factor_inverse, interface_block):
    layers, layer_rows = lax.axis_size("layer"), lax.axis_size("sub")
    cols_grid = lax.axis_size("pcol")
    width = interface_block.shape[-1]
    base = interface_block[0, :, 0]
    parts, start, side, side_start, inverse, slots = exchange(
        iface_tiles.T, interior_sizes, coupling[0], factor_inverse[0], base, layers, layer_rows, cols_grid
    )
    summed, panel, _ = subtract(
        slots,
        start.reshape(-1, width, width),
        parts.reshape(parts.shape[0], -1, width, width),
        side,
        side_start,
        inverse,
    )
    return (summed.reshape(interface_block.shape), panel[None])


def solution(mesh):
    rows_grid, cols_grid = mesh.shape["prow"], mesh.shape["pcol"]
    grid = Mesh(
        mesh.devices.reshape(LAYERS, rows_grid // LAYERS, cols_grid), ("layer", "sub", "pcol")
    )
    prow = ("layer", "sub")
    every = ("layer", "sub", "pcol")
    in_specs = (
        P(),
        P(every),
        P(every, None, None),
        P(every, None, None),
        P(prow, None, "pcol", None, None, None),
    )
    out_specs = (P(prow, None, "pcol", None, None, None), P(prow, None, "pcol", None))
    return jax.shard_map(shards, mesh=grid, in_specs=in_specs, out_specs=out_specs, check_vma=False)
```

```python
import functools

import jax
import jax.numpy as jnp
from jax import lax
from jax.experimental import pallas as pl
from jax.experimental.pallas import tpu as pltpu
from jax.sharding import Mesh, PartitionSpec as P

HIGHEST = lax.Precision.HIGHEST
MESH = pl.DeviceIdType.MESH
LAYERS = 4


def split(x):
    high = x.astype(jnp.bfloat16)
    low = (x - high.astype(jnp.float32)).astype(jnp.bfloat16)
    return high, low


def dot3(a_high, a_low, b_high, b_low):
    dot = functools.partial(jnp.dot, preferred_element_type=jnp.float32)
    return dot(a_high, b_high) + (dot(a_high, b_low) + dot(a_low, b_high))


def members(tiles_ref, row, count, modulus, residue, want):
    found, places = [jnp.int32(0)] * want, [jnp.int32(0)] * want
    seen = jnp.int32(0)
    for j in range(count):
        tile = tiles_ref[j, row]
        match = lax.rem(tile, modulus) == residue
        for k in range(want):
            hit = match & (seen == k)
            found[k] = jnp.where(hit, tile, found[k])
            places[k] = jnp.where(hit, jnp.int32(j), places[k])
        seen = seen + match.astype(jnp.int32)
    return found, places


def factor_inverse_of(matrix):
    size = matrix.shape[0]
    rows = lax.broadcasted_iota(jnp.int32, matrix.shape, 0)
    cols = lax.broadcasted_iota(jnp.int32, matrix.shape, 1)

    def eliminate(j, carry):
        rest, inverse = carry
        row = jnp.sum(jnp.where(rows == j, rest, 0.0), axis=0, keepdims=True)
        column = jnp.sum(jnp.where(cols == j, rest, 0.0), axis=1, keepdims=True)
        pivot = jnp.sum(jnp.where(cols[:1] == j, row, 0.0), axis=1, keepdims=True)
        scale = 1.0 / jnp.sqrt(pivot)
        below = jnp.where(rows[:, :1] > j, column * scale, 0.0)
        solved = jnp.sum(jnp.where(rows == j, inverse, 0.0), axis=0, keepdims=True) * scale
        rest = rest - below * (row * scale)
        inverse = jnp.where(rows == j, solved, inverse - below * solved)
        return rest, inverse

    return lax.fori_loop(0, size, eliminate, (matrix, (rows == cols).astype(jnp.float32)))[1]


def exchange_kernel(
    layers, layer_rows, cols_grid, rows_per, width,
    tiles_ref, sizes_ref, coupling_ref, factor_ref, base_ref,
    parts_ref, start_ref, side_ref, side_start_ref, inverse_ref, slots_ref,
    block_ref, corner_ref, w_ref, high_ref, low_ref, row_high_ref, row_low_ref, stage_ref, sums_ref, heard_ref,
    load_sem, base_sem, up_send, down_send, arrive, tile_send, tile_recv, side_send, side_recv, share_send, share_recv, sum_send, sum_recv,
):
    classes = layers * layer_rows
    group = layer_rows * cols_grid
    laps = classes // cols_grid
    tile_count = block_ref.shape[0]
    layer, sub, pcol = lax.axis_index("layer"), lax.axis_index("sub"), lax.axis_index("pcol")
    me = sub * cols_grid + pcol
    self_index = layer * group + me
    prow = layer * layer_rows + sub
    last = layers - 1
    block = rows_per * width
    local_cols = base_ref.shape[1]
    share = side_ref.shape[3]

    interior = factor_ref.shape[0]
    side = interior // width

    def factor_tile(n):
        rest, c = divmod(n, rows_per)
        rest, r = divmod(rest, rows_per)
        m, t = divmod(rest, layer_rows)
        return stage_ref.at[1, m, t, r, c]

    def spot(n):
        return slice(n // side * width, (n // side + 1) * width), slice(n % side * width, (n % side + 1) * width)

    loads = [pltpu.make_async_copy(base_ref.at[0, 0], corner_ref, load_sem.at[0])]
    for n in range(side * side):
        loads.append(pltpu.make_async_copy(factor_ref.at[spot(n)], factor_tile(n), load_sem.at[1 + n]))
    for j in range(tile_count):
        tile = coupling_ref.at[:, j * width : (j + 1) * width]
        loads.append(pltpu.make_async_copy(tile, block_ref.at[j], load_sem.at[1 + side * side + j]))
    for load in loads:
        load.start()
    preload = pltpu.make_async_copy(base_ref, start_ref, base_sem)

    barrier = pltpu.get_barrier_semaphore()

    def greet(k, carry):
        peer = lax.rem(me + k, group)
        pl.semaphore_signal(
            barrier, inc=1, device_id=(layer, peer // cols_grid, lax.rem(peer, cols_grid)), device_id_type=MESH
        )
        return carry

    lax.fori_loop(1, group, greet, 0)
    for other in (last - layer, layer ^ 1):
        pl.semaphore_signal(barrier, inc=1, device_id=(other, sub, pcol), device_id_type=MESH)

    first = jnp.int32(0)
    present = jnp.int32(0)
    for j in range(tile_count):
        hit = tiles_ref[j, self_index] == 0
        first = jnp.where(hit, jnp.int32(j), first)
        present = jnp.where(hit, jnp.int32(1), present)

    for load in loads:
        load.wait()
    for n in range(side * side):
        high, low = split(factor_tile(n)[...])
        row_high_ref[spot(n)] = high
        row_low_ref[spot(n)] = low
    size = sizes_ref[0]

    def weigh(columns, limit):
        live = lax.broadcasted_iota(jnp.int32, columns.shape, 0) < limit
        product = dot3(row_high_ref[:interior], row_low_ref[:interior], *split(jnp.where(live, columns, 0.0)))
        return jnp.where(live, product, 0.0)

    def up_copy(source, m, c):
        return pltpu.make_async_remote_copy(
            src_ref=w_ref.at[source, m, :, c * width : (c + 1) * width],
            dst_ref=w_ref.at[source, m, :, c * width : (c + 1) * width],
            send_sem=up_send.at[source, m, c],
            recv_sem=arrive.at[source, m, c],
            device_id=(jnp.minimum(layer + 1, last), sub, pcol),
            device_id_type=MESH,
        )

    def down_copy(source, m, c):
        return pltpu.make_async_remote_copy(
            src_ref=w_ref.at[source, m, :, c * width : (c + 1) * width],
            dst_ref=w_ref.at[source, m, :, c * width : (c + 1) * width],
            send_sem=down_send.at[source, m, c],
            recv_sem=arrive.at[source, m, c],
            device_id=(jnp.maximum(layer - 1, 0), sub, pcol),
            device_id_type=MESH,
        )

    def pass_up(source, m):
        @pl.when(layer < last)
        def _():
            for c in range(rows_per):
                up_copy(source, m, c).start()

    def pass_down(source, m):
        @pl.when(layer > 0)
        def _():
            for c in range(rows_per):
                down_copy(source, m, c).start()

    steps = sums_ref.shape[0] - 1

    def sum_copy(k):
        if k == 0:
            partner = (last - layer, sub, pcol)
        elif k == 1:
            partner = (layer ^ 1, sub, pcol)
        else:
            peer = me ^ (group >> (k - 1))
            partner = (layer, peer // cols_grid, lax.rem(peer, cols_grid))
        return pltpu.make_async_remote_copy(
            src_ref=sums_ref.at[k],
            dst_ref=heard_ref.at[k],
            send_sem=sum_send.at[k],
            recv_sem=sum_recv.at[k],
            device_id=partner,
            device_id_type=MESH,
        )

    def sum_up(k):
        sum_copy(k).wait()
        sums_ref[k + 1] = sums_ref[k] + heard_ref[k]

    def keep(m, product):
        high, low = split(product)
        high_ref[m] = high
        low_ref[m] = low

    def weigh_class(m):
        order = members(tiles_ref, self_index, tile_count, classes, m, rows_per)[1]
        product = weigh(jnp.concatenate([block_ref[at] for at in order], axis=1), size)
        w_ref[layer, m] = product
        keep(m, product)

    def share_copy(q):
        return pltpu.make_async_remote_copy(
            src_ref=base_ref.at[:, 0, q * share : (q + 1) * share, :],
            dst_ref=side_start_ref,
            send_sem=share_send.at[q],
            recv_sem=share_recv,
            device_id=(layer, sub, q),
            device_id_type=MESH,
        )

    own_share = pltpu.make_async_copy(base_ref.at[:, 0, :share, :], side_start_ref, share_send.at[0])

    middle = classes // 2

    def up_order(i):
        near_end = classes - layer_rows * (1 + i // layer_rows) + lax.rem(i, layer_rows)
        return jnp.where(i < middle, near_end, lax.rem(i + 1 + pcol, middle))

    def down_order(i):
        return jnp.where(i < middle, i, middle + lax.rem(i + 1 + pcol, middle))

    def weigh_pair(i):
        weigh_class(up_order(i))
        weigh_class(down_order(i))

    def pass_pair(i):
        pass_up(layer, up_order(i))
        pass_down(layer, down_order(i))

    weigh_pair(0)
    pl.semaphore_wait(barrier, group + 1)
    pass_pair(0)
    preload.start()
    product = weigh(block_ref[first], size * present)
    square = dot3(*split(product.T), *split(product))
    sums_ref[0] = jnp.where(self_index == 0, corner_ref[...], 0.0) - square

    sum_copy(0).start()

    @pl.when(pcol == 0)
    def _():
        own_share.start()
        for q in range(1, cols_grid):
            share_copy(q).start()

    weigh_pair(1)
    pass_pair(1)
    weigh_pair(2)
    sum_up(0)
    sum_copy(1).start()
    pass_pair(2)

    def weigh_rest(i, carry):
        weigh_pair(i)
        return carry

    lax.fori_loop(3, middle, weigh_rest, 0)
    sum_up(1)
    sum_copy(2).start()

    def pass_rest(i, carry):
        pass_pair(i)
        return carry

    lax.fori_loop(3, classes, pass_rest, 0)
    for k in range(2, steps):
        sum_up(k)
        if k + 1 < steps:
            sum_copy(k + 1).start()

    def tiles_out(source, m, slot, target):
        q, lap = lax.rem(m, cols_grid), m // cols_grid
        return pltpu.make_async_remote_copy(
            src_ref=stage_ref.at[slot, m, target],
            dst_ref=parts_ref.at[source * group + me, lap],
            send_sem=tile_send.at[slot, m, target],
            recv_sem=tile_recv.at[source * group + me, lap],
            device_id=(layer, target, q),
            device_id_type=MESH,
        )

    def tile_out(source, m, slot, target, c):
        q, lap = lax.rem(m, cols_grid), m // cols_grid
        return pltpu.make_async_remote_copy(
            src_ref=stage_ref.at[slot, m, target, :, c],
            dst_ref=parts_ref.at[source * group + me, lap, :, c],
            send_sem=tile_send.at[slot, m, target],
            recv_sem=tile_recv.at[source * group + me, lap],
            device_id=(layer, target, q),
            device_id_type=MESH,
        )

    def side_out(source, slot, target, p):
        return pltpu.make_async_remote_copy(
            src_ref=stage_ref.at[slot, 0, target, :, :, pl.ds(p * share, share), :],
            dst_ref=side_ref.at[source * group + me],
            send_sem=side_send.at[slot, target, p],
            recv_sem=side_recv.at[source * group + me],
            device_id=(layer, target, p),
            device_id_type=MESH,
        )

    def take_rows(source):
        for t in range(layer_rows):
            high, low = split(w_ref[source, layer * layer_rows + t].T)
            row_high_ref[t * block : (t + 1) * block] = high
            row_low_ref[t * block : (t + 1) * block] = low

    def column(source, m, slot, picked):
        q, lap = lax.rem(m, cols_grid), m // cols_grid
        span = slice(picked[0] * width, (picked[-1] + 1) * width)
        for t in range(layer_rows):
            rows = slice(t * block, (t + 1) * block)
            product = dot3(row_high_ref[rows], row_low_ref[rows], high_ref[m, :, span], low_ref[m, :, span])
            away = (q != pcol) | (sub != t)

            def write(ref):
                for r in range(rows_per):
                    for n, c in enumerate(picked):
                        ref[r, c] = product[r * width : (r + 1) * width, n * width : (n + 1) * width]

            @pl.when(away | (m == 0))
            def _():
                write(stage_ref.at[slot, m, t])

            @pl.when(away)
            def _():
                if len(picked) == rows_per:
                    tiles_out(source, m, slot, t).start()
                else:
                    for c in picked:
                        tile_out(source, m, slot, t, c).start()

            @pl.when(jnp.logical_not(away))
            def _():
                write(parts_ref.at[source * group + me, lap])

            @pl.when(m == 0)
            def _():
                for p in range(cols_grid):

                    @pl.when((p == pcol) & (sub == t))
                    def _():
                        for r in range(rows_per):
                            for n, c in enumerate(picked):
                                top = r * width + p * share
                                side_ref[source * group + me, r, c] = product[
                                    top : top + share, n * width : (n + 1) * width
                                ]

                    if picked[-1] == rows_per - 1:

                        @pl.when((p != pcol) | (sub != t))
                        def _():
                            side_out(source, slot, t, p).start()

    def sent(source, slot):
        def wait(n, carry):
            m, t = n // layer_rows, lax.rem(n, layer_rows)

            @pl.when((lax.rem(m, cols_grid) != pcol) | (sub != t))
            def _():
                tiles_out(source, m, slot, t).wait_send()

            return carry

        lax.fori_loop(0, classes * layer_rows, wait, 0)
        for t in range(layer_rows):
            for p in range(cols_grid):

                @pl.when((p != pcol) | (sub != t))
                def _():
                    side_out(source, slot, t, p).wait_send()

    def columns(source, slot, ordered, low, top):
        def step(i, carry):
            column(source, ordered(i), slot, tuple(range(rows_per)))
            return carry

        lax.fori_loop(low, top, step, 0)

    def straight(i):
        return i

    take_rows(layer)
    columns(layer, 0, straight, 0, classes)

    total = sums_ref[steps]
    inverse_ref[...] = factor_inverse_of(0.5 * (total + total.T))

    each = rows_per * laps * rows_per

    def place_tiles(sender, carry):
        row_tiles = members(tiles_ref, sender, tile_count, classes, prow, rows_per)[0]
        for lap in range(laps):
            col_tiles = members(tiles_ref, sender, tile_count, classes, lap * cols_grid + pcol, rows_per)[0]
            for r in range(rows_per):
                for c in range(rows_per):
                    slots_ref[sender * each + (lap * rows_per + r) * rows_per + c] = (
                        row_tiles[r] // classes * local_cols + col_tiles[c] // cols_grid
                    )
        zeros = members(tiles_ref, sender, tile_count, classes, 0, rows_per)[0]
        pick = jnp.int32(-1)
        for c in range(rows_per):
            pick = jnp.where(zeros[c] == 0, jnp.int32(c), pick)
        slots_ref[layers * group * each + sender] = pick
        return carry

    def up_onward(source, m, c):
        @pl.when(layer < last)
        def _():
            up_copy(source, m, c).start()

    def down_onward(source, m, c):
        @pl.when(layer > 0)
        def _():
            down_copy(source, m, c).start()

    def relay(i, carry):
        @pl.when(layer > 0)
        def _():
            source, m = layer - 1, up_order(i)
            for c in range(rows_per):
                up_copy(source, m, c).wait_recv()
                up_onward(source, m, c)

        @pl.when(layer < last)
        def _():
            source, m = layer + 1, down_order(i)
            for c in range(rows_per):
                down_copy(source, m, c).wait_recv()
                down_onward(source, m, c)

        return carry

    lax.fori_loop(0, classes, relay, 0)

    def absorb(source, slot):
        def prepare(m, carry):
            keep(m, w_ref[source, m])
            return carry

        lax.fori_loop(0, classes, prepare, 0)
        take_rows(source)
        columns(source, slot, straight, 0, classes)

    @pl.when(layer > 0)
    def _():
        absorb(layer - 1, 1)

    sent(layer, 0)

    @pl.when(layer < last)
    def _():
        absorb(layer + 1, 0)

    @pl.when(layer > 0)
    def _():
        sent(layer - 1, 1)

    rising = layer >= layers // 2

    def order(i):
        return jnp.where(rising, up_order(i), down_order(i))

    near = jnp.where(rising, layer - 1, layer + 1)
    second = jnp.where(rising, layer - 2, layer + 2)
    final = order(classes - 1)

    def stream(distance, slot, passing):
        source = jnp.where(rising, layer - distance, layer + distance)

        if passing:

            def settle(m, carry):
                for c in range(rows_per):

                    @pl.when(rising & (layer < last))
                    def _():
                        up_copy(near, m, c).wait_send()

                    @pl.when(jnp.logical_not(rising) & (layer > 0))
                    def _():
                        down_copy(near, m, c).wait_send()

                return carry

            lax.fori_loop(0, classes, settle, 0)

        def receive(i, c):
            m = order(i)
            up_copy(source, m, c).wait_recv()
            if passing:
                before = order(jnp.maximum(i - 1, 0))

                @pl.when(rising & (layer < last))
                def _():
                    @pl.when(i > 0)
                    def _():
                        up_copy(source, before, c).wait_send()

                    up_copy(source, m, c).start()

                @pl.when(jnp.logical_not(rising) & (layer > 0))
                def _():
                    @pl.when(i > 0)
                    def _():
                        down_copy(source, before, c).wait_send()

                    down_copy(source, m, c).start()

            half = slice(c * width, (c + 1) * width)
            high, low = split(w_ref[source, m, :, half])
            high_ref[m, :, half] = high
            low_ref[m, :, half] = low

        def gather(i, carry):
            for c in range(rows_per):
                receive(i, c)
            return carry

        lax.fori_loop(0, middle, gather, 0)
        take_rows(source)
        columns(source, slot, order, 0, middle)

        def step(i, carry):
            for c in range(rows_per):
                receive(i, c)
                column(source, order(i), slot, (c,))
            return carry

        lax.fori_loop(middle, classes, step, 0)

    stream(2, 1, True)
    lax.fori_loop(0, layers * group, place_tiles, 0)

    @pl.when(layer < last)
    def _():
        sent(layer + 1, 0)

    ends = (layer == 0) | (layer == last)

    def landed(source):
        def wait(k, carry):
            peer = lax.rem(me + k, group)
            for lap in range(laps):
                pltpu.make_async_remote_copy(
                    src_ref=stage_ref.at[0, 0, 0],
                    dst_ref=parts_ref.at[source * group + peer, lap],
                    send_sem=tile_send.at[0, 0, 0],
                    recv_sem=tile_recv.at[source * group + peer, lap],
                    device_id=(layer, peer // cols_grid, lax.rem(peer, cols_grid)),
                    device_id_type=MESH,
                ).wait_recv()
            pltpu.make_async_remote_copy(
                src_ref=stage_ref.at[0, 0, 0, :, :, pl.ds(0, share), :],
                dst_ref=side_ref.at[source * group + peer],
                send_sem=side_send.at[0, 0, 0],
                recv_sem=side_recv.at[source * group + peer],
                device_id=(layer, peer // cols_grid, lax.rem(peer, cols_grid)),
                device_id_type=MESH,
            ).wait_recv()

            return carry

        lax.fori_loop(1, group, wait, 0)

    @pl.when(pcol == 0)
    def _():
        own_share.wait()
        for q in range(1, cols_grid):
            share_copy(q).wait_send()

    @pl.when(pcol != 0)
    def _():
        share_copy(1).wait_recv()

    farthest = jnp.where(rising, layer - 3, layer + 3)

    def landed_early(source, carry):
        @pl.when(jnp.logical_not(ends) | (source != farthest))
        def _():
            landed(source)

        return carry

    lax.fori_loop(0, layers, landed_early, 0)
    sent(jnp.where(rising, layer - 2, layer + 2), 1)
    def passed(source, carry):
        def wait(m, inner):
            kept = (source != near) & ((source != second) | (m == final))

            @pl.when((source <= layer) & (layer < last) & kept)
            def _():
                for c in range(rows_per):
                    up_copy(source, m, c).wait_send()

            @pl.when((source >= layer) & (layer > 0) & kept)
            def _():
                for c in range(rows_per):
                    down_copy(source, m, c).wait_send()

            return inner

        return lax.fori_loop(0, classes, wait, carry)

    lax.fori_loop(0, layers, passed, 0)
    preload.wait()

    @pl.when(ends)
    def _():
        stream(3, 0, False)
        landed(farthest)
        sent(farthest, 0)


def exchange(tiles, sizes, coupling, factor, base, layers, layer_rows, cols_grid):
    interior, iface = coupling.shape
    width = base.shape[-1]
    classes = layers * layer_rows
    rows_per = iface // width // classes
    laps = classes // cols_grid
    group = layer_rows * cols_grid
    senders = layers * group
    parts = (senders, laps, rows_per, rows_per, width, width)
    chunks = (classes, interior, rows_per * width)
    steps = senders.bit_length() - 1
    share = width // cols_grid
    dma = pltpu.SemaphoreType.DMA
    vmem = pl.BlockSpec(memory_space=pltpu.VMEM)
    hbm = pl.BlockSpec(memory_space=pltpu.HBM)
    scalars = pl.BlockSpec(memory_space=pltpu.SMEM)
    return pl.pallas_call(
        functools.partial(exchange_kernel, layers, layer_rows, cols_grid, rows_per, width),
        in_specs=[scalars, scalars, hbm, hbm, hbm],
        out_specs=[vmem, vmem, vmem, vmem, vmem, scalars],
        out_shape=[
            pltpu.VMEM(parts, jnp.float32),
            pltpu.VMEM(base.shape, jnp.float32),
            pltpu.VMEM((senders, rows_per, rows_per, share, width), jnp.float32),
            pltpu.VMEM((base.shape[0], share, width), jnp.float32),
            pltpu.VMEM((width, width), jnp.float32),
            pltpu.SMEM((senders * (laps * rows_per * rows_per + 1),), jnp.int32),
        ],
        scratch_shapes=[
            pltpu.VMEM((iface // width, interior, width), jnp.float32),
            pltpu.VMEM((width, width), jnp.float32),
            pltpu.VMEM((layers, *chunks), jnp.float32),
            pltpu.VMEM(chunks, jnp.bfloat16),
            pltpu.VMEM(chunks, jnp.bfloat16),
            pltpu.VMEM((max(interior, iface // layers), interior), jnp.bfloat16),
            pltpu.VMEM((max(interior, iface // layers), interior), jnp.bfloat16),
            pltpu.VMEM((2, classes, layer_rows, rows_per, rows_per, width, width), jnp.float32),
            pltpu.VMEM((steps + 1, width, width), jnp.float32),
            pltpu.VMEM((steps, width, width), jnp.float32),
            dma((iface // width + (interior // width) ** 2 + 1,)), dma,
            dma((layers, classes, rows_per)), dma((layers, classes, rows_per)), dma((layers, classes, rows_per)),
            dma((2, classes, layer_rows)), dma((senders, laps)),
            dma((2, layer_rows, cols_grid)), dma((senders,)),
            dma((cols_grid,)), dma,
            dma((steps,)), dma((steps,)),
        ],
        compiler_params=pltpu.CompilerParams(
            vmem_limit_bytes=37 << 20, collective_id=0, has_side_effects=True
        ),
        name="exchange",
    )(tiles, sizes, *(pltpu.with_memory_space_constraint(x, pltpu.HBM) for x in (coupling, factor, base)))


def subtract_kernel(
    slots_ref, start_ref, parts_ref, side_ref, side_start_ref, inverse_ref,
    out_ref, panel_ref, sum_ref, column_ref, store_sem,
):
    senders, count = parts_ref.shape[:2]
    local_cols, rows_per = out_ref.shape[0] // side_start_ref.shape[0], side_ref.shape[1]

    def take(n, carry):
        for i in range(count):
            slot = slots_ref[n * count + i]
            sum_ref[slot] = sum_ref[slot] - parts_ref[n, i]
        return carry

    lax.fori_loop(0, senders, take, 0)
    local_rows = side_start_ref.shape[0]
    stores = []
    for a in range(local_rows):
        tiles = pl.ds(a * local_cols, local_cols)
        stores.append(pltpu.make_async_copy(sum_ref.at[tiles], out_ref.at[tiles], store_sem.at[1 + a]))
        stores[-1].start()
    column_ref[...] = side_start_ref[...]

    def pick(n, carry):
        chosen = slots_ref[senders * count + n]

        @pl.when(chosen >= 0)
        def _():
            for r in range(rows_per):
                slot = slots_ref[n * count + r * rows_per] // local_cols
                column_ref[slot] = column_ref[slot] - side_ref[n, r, chosen]

        return carry

    lax.fori_loop(0, senders, pick, 0)
    column = column_ref[...].reshape(-1, column_ref.shape[-1])
    panel = jnp.dot(column, inverse_ref[...].T, precision=HIGHEST, preferred_element_type=jnp.float32)
    column_ref[...] = panel.reshape(column_ref.shape)
    ready = pltpu.make_async_copy(column_ref, panel_ref, store_sem.at[0])
    ready.start()
    for store in stores:
        store.wait()
    ready.wait()


def subtract(slots, start, parts, side, side_start, inverse):
    vmem = pl.BlockSpec(memory_space=pltpu.VMEM)
    hbm = pl.BlockSpec(memory_space=pltpu.HBM)
    return pl.pallas_call(
        subtract_kernel,
        in_specs=[pl.BlockSpec(memory_space=pltpu.SMEM), vmem, vmem, vmem, vmem, vmem],
        out_specs=[hbm, hbm, vmem],
        out_shape=[
            pltpu.HBM(start.shape, jnp.float32),
            pltpu.HBM(side_start.shape, jnp.float32),
            pltpu.VMEM(start.shape, jnp.float32),
        ],
        input_output_aliases={1: 2},
        scratch_shapes=[pltpu.VMEM(side_start.shape, jnp.float32), pltpu.SemaphoreType.DMA((1 + side_start.shape[0],))],
        compiler_params=pltpu.CompilerParams(vmem_limit_bytes=2 << 20),
        cost_estimate=pl.CostEstimate(
            flops=parts.size, bytes_accessed=8 * parts.size + 4 * start.size, transcendentals=0
        ),
        name="subtract",
    )(slots, start, parts, side, side_start, inverse)


def shards(iface_tiles, interior_sizes, coupling, factor_inverse, interface_block):
    layers, layer_rows = lax.axis_size("layer"), lax.axis_size("sub")
    cols_grid = lax.axis_size("pcol")
    width = interface_block.shape[-1]
    base = interface_block[0, :, 0]
    parts, start, side, side_start, inverse, slots = exchange(
        iface_tiles.T, interior_sizes, coupling[0], factor_inverse[0], base, layers, layer_rows, cols_grid
    )
    summed, panel, _ = subtract(
        slots,
        start.reshape(-1, width, width),
        parts.reshape(parts.shape[0], -1, width, width),
        side,
        side_start,
        inverse,
    )
    return (summed.reshape(interface_block.shape), panel[None])


def solution(mesh):
    rows_grid, cols_grid = mesh.shape["prow"], mesh.shape["pcol"]
    grid = Mesh(
        mesh.devices.reshape(LAYERS, rows_grid // LAYERS, cols_grid), ("layer", "sub", "pcol")
    )
    prow = ("layer", "sub")
    every = ("layer", "sub", "pcol")
    in_specs = (
        P(),
        P(every),
        P(every, None, None),
        P(every, None, None),
        P(prow, None, "pcol", None, None, None),
    )
    out_specs = (P(prow, None, "pcol", None, None, None), P(prow, None, "pcol", None))
    return jax.shard_map(shards, mesh=grid, in_specs=in_specs, out_specs=out_specs, check_vma=False)
```
